8 devices in a mesh: rep: 1 (over z), dp: 8 (over x, y, core).
Axes of the slice: x: 2, y: 2, z: 1, core: 2. Of those that a mesh axis runs over, the one named last changes fastest.
Arguments:
- x: bfloat16 [8, 2048, 1024], P(('rep', 'dp'))
- dy: bfloat16 [8, 2048, 1024], P(('rep', 'dp'))
- w_gate: bfloat16 [2, 1024, 2560], replicated
- w_up: bfloat16 [2, 1024, 2560], replicated
- w_down: bfloat16 [2, 2560, 1024], replicated
- m_w_gate: float32 [2, 1024, 2560], replicated
- m_w_up: float32 [2, 1024, 2560], replicated
- m_w_down: float32 [2, 2560, 1024], replicated
- v_w_gate: float32 [2, 1024, 2560], replicated
- v_w_up: float32 [2, 1024, 2560], replicated
- v_w_down: float32 [2, 2560, 1024], replicated
Outputs:
- output 1: bfloat16 [2, 1024, 2560], P('rep')
- output 2: bfloat16 [2, 1024, 2560], P('rep')
- output 3: bfloat16 [2, 2560, 1024], P('rep')
- output 4: float32 [2, 1024, 2560], P('rep')
- output 5: float32 [2, 1024, 2560], P('rep')
- output 6: float32 [2, 2560, 1024], P('rep')
- output 7: float32 [2, 1024, 2560], P('rep')
- output 8: float32 [2, 1024, 2560], P('rep')
- output 9: float32 [2, 2560, 1024], P('rep')
All inputs are finite; a program needn't handle non-finite values.
Results may differ from the reference program's by a relative error of at most 0.022.
Values are sent between devices in bfloat16 or wider.
A program may use at most 2.5 GiB of HBM per device.

```python
import jax
import jax.numpy as jnp
from jax import lax

SEQUENCES = 8
TOKENS = 2048
D = 1024
FF = 2560
LAYERS = 2
NAMES = ("w_gate", "w_up", "w_down")
SHAPES = {"w_gate": (LAYERS, D, FF), "w_up": (LAYERS, D, FF), "w_down": (LAYERS, FF, D)}


def bump(key, n, height):
    away = (jnp.arange(n, dtype=jnp.int32) - jax.random.randint(key, (), 0, n, jnp.int32)) % n
    return jnp.where(away < n // 8, height, 1.0)


def together(key, own, strength):
    shared = jax.random.normal(key, own.shape[1:], jnp.float32)
    return (own + strength * shared) * lax.rsqrt(1 + strength * strength)


def setup_inputs(seed: int = 0, part: int = 0) -> dict:
    kx, kdy, ka, kb, kz, kf, kh, kl, *keys = jax.random.split(jax.random.key(seed), 8 + 3 * len(NAMES))
    kx, kdy, ka, kb = (jax.random.fold_in(k, part) for k in (kx, kdy, ka, kb))
    kw, km, kv = (keys[i::3] for i in range(3))
    shape = (SEQUENCES, TOKENS, D)
    much_x, much_dy = jax.random.uniform(kz, (2,), jnp.float32, 0.0, 1.0)
    loud = 2.0 ** jax.random.uniform(jax.random.fold_in(kz, 1), (), jnp.float32, -1.0, 2.0)
    layers = 2.0 ** jax.random.uniform(kl, (LAYERS, 1, 1), jnp.float32, -1.0, 1.0)
    x = together(ka, jax.random.normal(kx, shape, jnp.float32), much_x) * bump(kf, D, 4.0)
    dy = together(kb, jax.random.normal(kdy, shape, jnp.float32), much_dy)
    drawn = {"x": x.astype(jnp.bfloat16), "dy": (loud * dy * (SEQUENCES * TOKENS) ** -0.5).astype(jnp.bfloat16)}
    for key, name in zip(kw, NAMES, strict=True):
        w = jax.random.normal(key, SHAPES[name], jnp.float32) * SHAPES[name][1] ** -0.5
        drawn[name] = (w * {"w_gate": 1.0, "w_up": bump(kh, FF, 4.0), "w_down": layers}[name]).astype(jnp.bfloat16)
    for key, name in zip(km, NAMES, strict=True):
        drawn[f"m_{name}"] = 0.1 * jax.random.normal(key, SHAPES[name], jnp.float32)
    for key, name in zip(kv, NAMES, strict=True):
        drawn[f"v_{name}"] = jax.random.uniform(key, SHAPES[name], jnp.float32, 0.005, 0.015)
    return drawn


def matmul(a, w):
    return jnp.dot(a, w, preferred_element_type=jnp.float32).astype(jnp.bfloat16)


def normed(h):
    wide = h.astype(jnp.float32)
    scale = lax.rsqrt(jnp.mean(wide**2, -1, keepdims=True) + 1e-6)
    return (wide * scale).astype(jnp.bfloat16)


def layer(h, w):
    a = normed(h)
    gate = jnp.dot(a, w["w_gate"], preferred_element_type=jnp.float32)
    up = jnp.dot(a, w["w_up"], preferred_element_type=jnp.float32)
    return h + matmul((jax.nn.silu(gate) * up).astype(jnp.bfloat16), w["w_down"])


def adamw(w, m, v, g):
    m = 0.9 * m + 0.1 * g
    v = 0.95 * v + 0.05 * g * g
    step = m * lax.rsqrt(v + 1e-8) + 0.1 * w
    return (w - 0.02 * step).astype(jnp.bfloat16), m, v


def clipped(gradients, sum_of_squares, count):
    factor = jnp.minimum(1.0, 0.5 * lax.rsqrt(sum_of_squares / count + 1e-30))
    return [g * factor for g in gradients]


def stack(weights, h):
    return lax.scan(lambda h, w: (layer(h, w), None), h, weights)[0]


def reference(x, dy, w_gate, w_up, w_down, m_w_gate, m_w_up, m_w_down, v_w_gate, v_w_up, v_w_down):
    weights = dict(zip(NAMES, (w_gate, w_up, w_down), strict=True))

    def take(so_far, sequence):
        h, by_y = sequence
        _, back = jax.vjp(lambda w: stack(w, h), weights)
        return jax.tree.map(lambda total, term: total + term.astype(jnp.float32), so_far, back(by_y)[0]), None

    none_yet = {name: jnp.zeros(w.shape, jnp.float32) for name, w in weights.items()}
    by_weights, _ = lax.scan(take, none_yet, (x, dy))
    gradients = [by_weights[name].astype(jnp.bfloat16).astype(jnp.float32) for name in NAMES]
    gradients = clipped(gradients, sum(jnp.sum(g * g) for g in gradients), sum(g.size for g in gradients))
    new = [
        adamw(w.astype(jnp.float32), m, v, g)
        for w, m, v, g in zip((w_gate, w_up, w_down), (m_w_gate, m_w_up, m_w_down), (v_w_gate, v_w_up, v_w_down), gradients, strict=True)
    ]
    return tuple(one[which] for which in range(3) for one in new)
```

```python
import jax
import jax.numpy as jnp
from jax import lax
from jax.experimental import pallas as pl
from jax.experimental.pallas import tpu as pltpu
from jax.sharding import PartitionSpec as P


T, D, F, L = 2048, 1024, 2560, 2
FT = 256
BLK = 128
SUB = 512
HALVES = (0, F // 2)
WIDE = F // 2
F32, BF16 = jnp.float32, jnp.bfloat16
MB = 1 << 20

NT = (((1,), (1,)), ((), ()))


def dot(a, b):
    return jnp.dot(a, b, preferred_element_type=F32)


def dot_nt(a, b):
    return lax.dot_general(a, b, NT, preferred_element_type=F32)


def sigmoid(x):
    return 0.5 * jnp.tanh(0.5 * x) + 0.5


def normed(h):
    wide = h.astype(F32)
    scale = lax.rsqrt(jnp.mean(wide * wide, -1, keepdims=True) + 1e-6)
    return (wide * scale).astype(BF16)


def place(shard, me):
    s = shard ^ me
    sx, sy, half = (s >> 2) & 1, (s >> 1) & 1, s & 1
    core = shard & 1
    return half * 4 + (1 - core) * (sx * 2 + sy) + core * (sy * 2 + sx)


def shard_at(p, me):
    half, k = p >> 2, p & 3
    hi, lo = k >> 1, k & 1
    core = (me & 1) ^ half
    sx, sy = (1 - core) * hi + core * lo, (1 - core) * lo + core * hi
    return me ^ (sx * 4 + sy * 2 + half)


def store_turned(me, tile, out_ref):
    for shard in range(8):
        rows = pl.ds(pl.multiple_of(place(jnp.int32(shard), me) * BLK, BLK), BLK)
        out_ref[rows, :] = tile[:, shard * BLK : (shard + 1) * BLK].T


def call(kernel, grid, ins, outs, scratch=(), flops=0, moved=0, aliases=None):
    return pl.pallas_call(
        kernel,
        grid_spec=pltpu.PrefetchScalarGridSpec(num_scalar_prefetch=1, grid=grid, in_specs=[s for s in ins], out_specs=[s for s, _ in outs], scratch_shapes=list(scratch)),
        out_shape=[o for _, o in outs],
        compiler_params=pltpu.CompilerParams(dimension_semantics=("arbitrary",) * len(grid), vmem_limit_bytes=63 * MB),
        cost_estimate=pl.CostEstimate(flops=int(flops), bytes_accessed=int(moved), transcendentals=0),
        input_output_aliases=aliases or {},
    )


def shaped(shape, dtype=BF16):
    return jax.ShapeDtypeStruct(shape, dtype)


MM = 2 * T * D * F


def prep(me, x, dy):
    rows = 256

    def kernel(me_ref, x_ref, dy_ref, a_ref, at_ref, dyt_ref):
        a = normed(x_ref[...])
        a_ref[...] = a
        store_turned(me_ref[0], a, at_ref)
        store_turned(me_ref[0], dy_ref[...], dyt_ref)

    tall = pl.BlockSpec((rows, D), lambda i, m: (i, 0))
    wide = pl.BlockSpec((D, rows), lambda i, m: (0, i))
    return call(kernel, (T // rows,), [tall, tall], [(tall, shaped((T, D))), (wide, shaped((D, T))), (wide, shaped((D, T)))], flops=MM // 3, moved=20e6)(me, x, dy)


def gate_up(me, a, w_gate, w_up):
    def kernel(me_ref, a_ref, wg_ref, wu_ref, g_ref, u_ref, act_ref):
        for t in range(T // SUB):
            rows = slice(t * SUB, (t + 1) * SUB)
            g = dot(a_ref[rows], wg_ref[0])
            u = dot(a_ref[rows], wu_ref[0])
            g_ref[rows, :] = g
            u_ref[rows, :] = u
            act_ref[rows, :] = (g * sigmoid(g) * u).astype(BF16)

    weight = pl.BlockSpec((1, D, FT), lambda j, m: (0, 0, j))
    tile = pl.BlockSpec((T, FT), lambda j, m: (0, j))
    return call(
        kernel,
        (F // FT,),
        [pl.BlockSpec((T, D), lambda j, m: (0, 0)), weight, weight],
        [(tile, shaped((T, F), F32)), (tile, shaped((T, F), F32)), (tile, shaped((T, F)))],
        flops=2 * MM,
        moved=67e6,
    )(me, a, w_gate, w_up)


def down(me, act, w_down, h):
    rows = 512

    def kernel(me_ref, act_ref, wd_ref, h_ref, out_ref, a_ref, at_ref):
        out = h_ref[...] + dot(act_ref[...], wd_ref[0]).astype(BF16)
        out_ref[...] = out
        a = normed(out)
        a_ref[...] = a
        store_turned(me_ref[0], a, at_ref)

    tall = pl.BlockSpec((rows, D), lambda i, m: (i, 0))
    return call(
        kernel,
        (T // rows,),
        [pl.BlockSpec((rows, F), lambda i, m: (i, 0)), pl.BlockSpec((1, F, D), lambda i, m: (0, 0, 0), pipeline_mode=pl.Buffered(1)), tall],
        [(tall, shaped((T, D))), (tall, shaped((T, D))), (pl.BlockSpec((D, rows), lambda i, m: (0, i)), shaped((D, T)))],
        flops=MM,
        moved=32e6,
    )(me, act, w_down, h)


def both(a, b):
    return (a.astype(F32) + b.astype(F32)).astype(BF16)


def grads(layer, a, at, dh, dht, w_gate, w_up, w_down, kept=None):
    make = kept is None
    n = F // FT

    def kernel(*refs):
        refs = list(refs)
        take = lambda count: [refs.pop(0) for _ in range(count)]
        hbm = take(4 if make else 3)
        (wd_ref,) = take(1)
        one, two = take(2)
        own_ref, sq_ref = take(2)
        dg_ref, du_ref = take(2)
        (act_ref,) = take(1)
        mine = take(len(hbm))
        keep, send, recv0, away1, stay1, recv1, away2, stay2, recv2 = take(9)
        sems, s0, r0, s1, r1, s2, r2 = take(7)
        copies = [pltpu.make_async_copy(s, d, sems.at[i]) for i, (s, d) in enumerate(zip(hbm, mine))]
        if make:
            dh_v, a_v, at_v, dht_v = mine
        else:
            dh_v, at_v, dht_v = mine
        early = 2 if make else 1
        j = pl.program_id(0)
        me = lax.axis_index("dp")
        core = me % 2
        other = me + 1 - 2 * core
        xs, ys = me + 4 - 8 * (me // 4), me + 2 - 4 * ((me // 2) % 2)
        near, far = (1 - core) * xs + core * ys, (1 - core) * ys + core * xs

        def remote(src, dst, ss, rs, to):
            return pltpu.make_async_remote_copy(src, dst, ss, rs, device_id={"dp": to}, device_id_type=pl.DeviceIdType.MESH)

        def core_copy(t):
            return remote(send.at[t % 2], recv0.at[t % 2], s0.at[t % 2], r0.at[t % 2], other)

        def near_copy(t):
            return remote(away1.at[t % 2], recv1.at[t % 4], s1.at[t % 2], r1.at[t % 4], near)

        def far_copy(t):
            return remote(away2.at[t % 2], recv2.at[t % 4], s2.at[t % 2], r2.at[t % 4], far)

        barrier = pltpu.get_barrier_semaphore()

        @pl.when(j == 0)
        def _():
            for to in (other, xs, ys):
                pl.semaphore_signal(barrier, inc=1, device_id={"dp": to}, device_id_type=pl.DeviceIdType.MESH)
            for c in copies:
                c.start()
            sq_ref[...] = jnp.zeros_like(sq_ref)

        @pl.when(j >= 6)
        def _():
            t = j - 6
            far_copy(t).wait()
            for i in range(3):
                done = both(stay2[t % 2, i], recv2[t % 4, i])
                own_ref[i] = done
                done = done.astype(F32)
                done = jnp.sum((done * done).reshape(BLK // 8, 8, FT), 0)
                sq_ref[...] += done[:, :128] + done[:, 128:]

        @pl.when((j >= 4) & (j < n + 4))
        def _():
            t = j - 4
            near_copy(t).wait()
            for i in range(3):
                away2[t % 2, i] = both(stay1[t % 2, 1, i], recv1[t % 4, 1, i])
                stay2[t % 2, i] = both(stay1[t % 2, 0, i], recv1[t % 4, 0, i])

        @pl.when((j >= 2) & (j < n + 2))
        def _():
            t = j - 2
            core_copy(t).wait()
            for k in range(2):
                for i in range(3):
                    away1[t % 2, k, i] = both(keep[t % 2, 2 + k, i], recv0[t % 2, 2 + k, i])
                    stay1[t % 2, k, i] = both(keep[t % 2, k, i], recv0[t % 2, k, i])

        def tokens(t):
            rows = slice(t * SUB, (t + 1) * SUB)
            if make:
                g, u = dot(a_v[rows], one[0]), dot(a_v[rows], two[0])
            else:
                g, u = one[rows, :], two[rows, :]
            dact = dot_nt(dh_v[rows], wd_ref[0]).astype(BF16).astype(F32)
            s = sigmoid(g)
            gs = g * s
            act_ref[rows, :] = (gs * u).astype(BF16)
            du_ref[rows, :] = (dact * gs).astype(BF16)
            dg_ref[rows, :] = (dact * u * (s + gs * (1.0 - s))).astype(BF16)

        @pl.when(j == 0)
        def _():
            for c in copies[:early]:
                c.wait()

        @pl.when(j < n)
        def _():
            tokens(0)

        @pl.when(j == 0)
        def _():
            pl.semaphore_wait(barrier, 3)

        @pl.when((j >= 4) & (j < n + 4))
        def _():
            far_copy(j - 4).start()

        @pl.when((j >= 2) & (j < n + 2))
        def _():
            near_copy(j - 2).start()

        @pl.when((j >= 1) & (j < n + 1))
        def _():
            core_copy(j - 1).start()

        @pl.when(j < n)
        def _():
            for t in range(1, T // SUB):
                tokens(t)

        @pl.when(j == 0)
        def _():
            for c in copies[early:]:
                c.wait()

        @pl.when(j < n)
        def _():
            for i, (left, right) in enumerate(((at_v, dg_ref), (at_v, du_ref), (dht_v, act_ref))):
                for half, out in enumerate((keep, send)):
                    made = dot(left[half * 4 * BLK : (half + 1) * 4 * BLK, :], right[...]).astype(BF16)
                    for k in range(4):
                        out[j % 2, k, i] = made[k * BLK : (k + 1) * BLK]

    last = n - 1
    whole = pl.BlockSpec(memory_space=pl.ANY)
    weight = pl.BlockSpec((1, D, FT), lambda j: (layer, 0, jnp.minimum(j, last)))
    wdown = pl.BlockSpec((1, FT, D), lambda j: (layer, jnp.minimum(j, last), 0))
    tile = pl.BlockSpec((T, FT), lambda j: (0, jnp.minimum(j, last)))
    outs = [
        (pl.BlockSpec((3, BLK, FT), lambda j: (0, 0, jnp.clip(j - 6, 0, last))), shaped((3, BLK, F))),
        (pl.BlockSpec((8, 128), lambda j: (0, 0)), shaped((8, 128), F32)),
    ]
    temp = pltpu.VMEM((T, FT), BF16)
    if make:
        args = [dh, a, at, dht, w_down, w_gate, w_up]
        ins = [whole] * 4 + [wdown, weight, weight]
        outs += [(tile, shaped((T, F)))] * 2
        scratch = [temp] + [pltpu.VMEM((T, D), BF16)] * 2 + [pltpu.VMEM((D, T), BF16)] * 2
    else:
        args = [dh, at, dht, w_down, *kept]
        ins = [whole] * 3 + [wdown, tile, tile]
        scratch = [temp] * 3 + [pltpu.VMEM((T, D), BF16)] + [pltpu.VMEM((D, T), BF16)] * 2
    quarter = lambda *lead: pltpu.VMEM((*lead, 3, BLK, FT), BF16)
    scratch += [quarter(2, 4), quarter(2, 4), quarter(2, 4), quarter(2, 2), quarter(2, 2), quarter(4, 2), quarter(2), quarter(2), quarter(4)]
    sem = pltpu.SemaphoreType.DMA
    scratch += [sem((4 if make else 3,)), sem((2,)), sem((2,)), sem((2,)), sem((4,)), sem((2,)), sem((4,))]
    return pl.pallas_call(
        kernel,
        grid_spec=pltpu.PrefetchScalarGridSpec(num_scalar_prefetch=0, grid=(n + 6,), in_specs=ins, out_specs=[s for s, _ in outs], scratch_shapes=scratch),
        out_shape=[o for _, o in outs],
        compiler_params=pltpu.CompilerParams(
            dimension_semantics=("arbitrary",), vmem_limit_bytes=63 * MB, collective_id=layer, has_side_effects=True
        ),
        cost_estimate=pl.CostEstimate(flops=(6 if make else 4) * MM, bytes_accessed=60_000_000, transcendentals=0),
    )(*args)


def back(me, dg, du, w_gate, w_up, h, dh):
    rows = 512

    def kernel(me_ref, dg_ref, du_ref, wg_ref, wu_ref, h_ref, dh_ref, out_ref, outt_ref):
        da = (dot_nt(dg_ref[...], wg_ref[0]) + dot_nt(du_ref[...], wu_ref[0])).astype(BF16).astype(F32)
        wide = h_ref[...].astype(F32)
        scale = lax.rsqrt(jnp.mean(wide * wide, -1, keepdims=True) + 1e-6)
        along = jnp.mean(da * wide, -1, keepdims=True) * (scale * scale * scale)
        out = dh_ref[...] + (da * scale - wide * along).astype(BF16)
        out_ref[...] = out
        store_turned(me_ref[0], out, outt_ref)

    tall = pl.BlockSpec((rows, D), lambda i, m: (i, 0))
    broad = pl.BlockSpec((rows, F), lambda i, m: (i, 0))
    weight = pl.BlockSpec((1, D, F), lambda i, m: (1, 0, 0), pipeline_mode=pl.Buffered(1))
    return call(
        kernel,
        (T // rows,),
        [broad, broad, weight, weight, tall, tall],
        [(tall, shaped((T, D))), (pl.BlockSpec((D, rows), lambda i, m: (0, i)), shaped((D, T)))],
        flops=2 * MM,
        moved=48e6,
    )(me, dg, du, w_gate, w_up, h, dh)


def adamw(me, layer, first, factor, parts, w, m, v, so_far):
    ft = 640
    steps, at0 = WIDE // ft, first // ft

    def kernel(me_ref, f_ref, *refs):
        parts, refs = refs[:8], refs[8:]
        ws, ms, vs = refs[0:3], refs[3:6], refs[6:9]
        nws, nms, nvs, part = refs[-10:-7], refs[-7:-4], refs[-4:-1], refs[-1]
        f = f_ref[0, 0]
        p = pl.program_id(0)
        for at in range(8):

            @pl.when(p == at)
            def _(at=at):
                part[...] = parts[at][...]

        def take(i, rows, g):
            g = g.astype(F32) * f
            new_m = 0.9 * ms[i][0, rows, :] + 0.1 * g
            new_v = 0.95 * vs[i][0, rows, :] + 0.05 * g * g
            wide = ws[i][0, rows, :].astype(F32)
            nws[i][0, rows, :] = (wide - 0.02 * (new_m * lax.rsqrt(new_v + 1e-8) + 0.1 * wide)).astype(BF16)
            nms[i][0, rows, :] = new_m
            nvs[i][0, rows, :] = new_v

        for r in range(0, BLK, 16):
            for i in range(2):
                take(i, slice(r, r + 16), part[i, r : r + 16, :])
        for r in range(0, ft, 128):
            take(2, slice(r, r + 128), part[2, :, r : r + 128].T)

    def piece(at):
        return pl.BlockSpec((3, BLK, ft), lambda p, j, me_ref: (0, 0, jnp.where(p == at, j, jnp.where(p < at, 0, steps - 1))))

    across = pl.BlockSpec((1, BLK, ft), lambda p, j, me_ref: (layer, shard_at(p, me_ref[0]), at0 + j))
    along = pl.BlockSpec((1, ft, BLK), lambda p, j, me_ref: (layer, at0 + j, shard_at(p, me_ref[0])))
    three = [across, across, along]
    whole = pl.BlockSpec(memory_space=pl.ANY)
    ins = [pl.BlockSpec(memory_space=pltpu.SMEM)] + [piece(at) for at in range(8)] + three * 3
    args = [factor] + list(parts) + list(w) + list(m) + list(v)
    outs = [(s, shaped(o.shape, o.dtype)) for s, o in zip(three * 3, list(w) + list(m) + list(v))]
    aliases = {}
    if so_far is not None:
        aliases = {1 + len(ins) + i: i for i in range(9)}
        ins, args = ins + [whole] * 9, args + list(so_far)
    size = 3 * WIDE * D
    return call(kernel, (8, steps), ins, outs, [pltpu.VMEM((3, BLK, ft), BF16)], flops=size * 200, moved=size * 22, aliases=aliases)(me, *args)


CORE = [(i, i ^ 1) for i in range(8)]
FIRST = [(i, i ^ (2 if i & 1 else 4)) for i in range(8)]
SECOND = [(i, i ^ (4 if i & 1 else 2)) for i in range(8)]


STAGES = {"core": CORE, "first": FIRST, "second": SECOND}


def swap(a, stage):
    return lax.ppermute(a, "dp", STAGES[stage])


def gather(own):
    mine = [own, swap(own, "second")]
    mine += [swap(a, "first") for a in mine]
    return mine + [swap(a, "core") for a in mine]


def solution(mesh):
    def work(x, dy, *arrays):
        weights, m, v = (arrays[i : i + 3] for i in (0, 3, 6))
        w_gate, w_up, w_down = weights
        x, dy = x[0], dy[0]
        me = lax.axis_index("dp").astype(jnp.int32).reshape(1)
        a0, a0t, dyt = prep(me, x, dy)
        gate, up, act = gate_up(me, a0, w_gate, w_up)
        h, a1, a1t = down(me, act, w_down, x)

        own1, squares1, dg, du = grads(1, a1, a1t, dy, dyt, *weights)
        dh, dht = back(me, dg, du, w_gate, w_up, h, dy)
        own0, squares0 = grads(0, a0, a0t, dh, dht, *weights, kept=(gate, up))

        squares = lax.psum(jnp.sum(squares1 + squares0), "dp")
        factor = jnp.minimum(1.0, 0.5 * lax.rsqrt(squares / (3 * L * D * F) + 1e-30)).reshape(1, 1)

        new = None
        for layer, own in ((1, own1), (0, own0)):
            for first in HALVES:
                parts = gather(own[:, :, first : first + WIDE])
                new = adamw(me, layer, first, factor, parts, weights, m, v, new)
        return tuple(new)

    return jax.shard_map(
        work,
        mesh=mesh,
        in_specs=(P(("rep", "dp"), None, None),) * 2 + (P(None, None, None),) * 9,
        out_specs=(P("rep", None, None),) * 9,
        check_vma=False,
    )
```

```python
import jax
import jax.numpy as jnp
from jax import lax
from jax.experimental import pallas as pl
from jax.experimental.pallas import tpu as pltpu
from jax.sharding import PartitionSpec as P


T, D, F, L = 2048, 1024, 2560, 2
FT = 256
BLK = 128
SUB = 512
HALVES = (0, F // 2)
WIDE = F // 2
F32, BF16 = jnp.float32, jnp.bfloat16
MB = 1 << 20

NT = (((1,), (1,)), ((), ()))


def dot(a, b):
    return jnp.dot(a, b, preferred_element_type=F32)


def dot_nt(a, b):
    return lax.dot_general(a, b, NT, preferred_element_type=F32)


def sigmoid(x):
    return 0.5 * jnp.tanh(0.5 * x) + 0.5


def normed(h):
    wide = h.astype(F32)
    scale = lax.rsqrt(jnp.mean(wide * wide, -1, keepdims=True) + 1e-6)
    return (wide * scale).astype(BF16)


def place(shard, me):
    sx, sy, half = (flip + (1 - 2 * flip) * bit for bit, flip in zip((me // 4, (me // 2) % 2, me % 2), (shard >> 2, (shard >> 1) & 1, shard & 1)))
    return half * 4 + (sy * 2 + sx if shard & 1 else sx * 2 + sy)


def shard_at(p, me):
    half, k = p >> 2, p & 3
    hi, lo = k >> 1, k & 1
    core = (me & 1) ^ half
    sx, sy = (1 - core) * hi + core * lo, (1 - core) * lo + core * hi
    return me ^ (sx * 4 + sy * 2 + half)


def store_turned(me, tile, out_ref, columns=slice(None)):
    for shard in range(8):
        rows = pl.ds(pl.multiple_of(place(shard, me) * BLK, BLK), BLK)
        out_ref[rows, columns] = tile[:, shard * BLK : (shard + 1) * BLK].T


def call(kernel, grid, ins, outs, scratch=(), flops=0, moved=0, aliases=None):
    return pl.pallas_call(
        kernel,
        grid_spec=pltpu.PrefetchScalarGridSpec(num_scalar_prefetch=1, grid=grid, in_specs=[s for s in ins], out_specs=[s for s, _ in outs], scratch_shapes=list(scratch)),
        out_shape=[o for _, o in outs],
        compiler_params=pltpu.CompilerParams(dimension_semantics=("arbitrary",) * len(grid), vmem_limit_bytes=63 * MB),
        cost_estimate=pl.CostEstimate(flops=int(flops), bytes_accessed=int(moved), transcendentals=0),
        input_output_aliases=aliases or {},
    )


def shaped(shape, dtype=BF16):
    return jax.ShapeDtypeStruct(shape, dtype)


MM = 2 * T * D * F


def gate_up(me, x, w_gate, w_up):
    def kernel(me_ref, x_ref, wg_ref, wu_ref, g_ref, u_ref, act_ref, a_ref):
        @pl.when(pl.program_id(0) == 0)
        def _():
            for t in range(T // SUB):
                rows = slice(t * SUB, (t + 1) * SUB)
                a_ref[rows, :] = normed(x_ref[rows, :])

        for t in range(T // SUB):
            rows = slice(t * SUB, (t + 1) * SUB)
            g = dot(a_ref[rows], wg_ref[0])
            u = dot(a_ref[rows], wu_ref[0])
            g_ref[rows, :] = g
            u_ref[rows, :] = u
            act_ref[rows, :] = (g * sigmoid(g) * u).astype(BF16)

    weight = pl.BlockSpec((1, D, FT), lambda j, m: (0, 0, j))
    tile = pl.BlockSpec((T, FT), lambda j, m: (0, j))
    return call(
        kernel,
        (F // FT,),
        [pl.BlockSpec((T, D), lambda j, m: (0, 0), pipeline_mode=pl.Buffered(1)), weight, weight],
        [(tile, shaped((T, F), F32)), (tile, shaped((T, F), F32)), (tile, shaped((T, F)))],
        [pltpu.VMEM((T, D), BF16)],
        flops=2 * MM,
        moved=67e6,
    )(me, x, w_gate, w_up)


def down(me, act, w_down, x, dy):
    rows = 512

    def kernel(me_ref, act_ref, wd_ref, x_ref, dy_ref, out_ref, a_ref, at_ref, a0t_ref, dyt_ref):
        store_turned(me_ref[0], normed(x_ref[...]), a0t_ref)
        store_turned(me_ref[0], dy_ref[...], dyt_ref)
        out = x_ref[...] + dot(act_ref[...], wd_ref[0]).astype(BF16)
        out_ref[...] = out
        a = normed(out)
        a_ref[...] = a
        store_turned(me_ref[0], a, at_ref)

    tall = pl.BlockSpec((rows, D), lambda i, m: (i, 0))
    flat = pl.BlockSpec((D, rows), lambda i, m: (0, i))
    return call(
        kernel,
        (T // rows,),
        [pl.BlockSpec((rows, F), lambda i, m: (i, 0)), pl.BlockSpec((1, F, D), lambda i, m: (0, 0, 0), pipeline_mode=pl.Buffered(1)), tall, tall],
        [(tall, shaped((T, D))), (tall, shaped((T, D)))] + [(flat, shaped((D, T)))] * 3,
        flops=MM,
        moved=44e6,
    )(me, act, w_down, x, dy)


def both(a, b):
    return (a.astype(F32) + b.astype(F32)).astype(BF16)


def backward(dy, a1, a1t, dyt, h, a0t, gate, up, w_gate, w_up, w_down):
    n = F // FT
    mid = n // 2
    turn, low = n, n + 1
    end = low + n
    steps = end + 7

    def kernel(*refs):
        refs = list(refs)
        take = lambda count: [refs.pop(0) for _ in range(count)]
        dy_ref, a1_ref, a1t_ref, dyt_ref, h_ref, a0t_ref = take(6)
        wd_ref, wg_ref, wu_ref, g_ref, u_ref = take(5)
        owns = take(4)
        got_ref, factor_ref = take(2)
        dg_ref, du_ref, act_ref = take(3)
        dh_v, a_v, at_v, dht_v, acc = take(5)
        keep, send, recv0, away1, stay1, recv1, away2, stay2, recv2, own_v = take(10)
        sq_ref, all_sq = take(2)
        sems, s0, r0, s1, r1, s2, r2, s3, r3, s4, r4, s5, r5, s6, r6 = take(15)
        pairs = ((dy_ref, dh_v), (a1_ref, a_v), (a1t_ref, at_v), (dyt_ref, dht_v), (h_ref, a_v), (a0t_ref, at_v))
        copies = [pltpu.make_async_copy(s, d, sems.at[i]) for i, (s, d) in enumerate(pairs)]
        j = pl.program_id(0)
        me = lax.axis_index("dp")
        core = me % 2
        other = me + 1 - 2 * core
        xs, ys = me + 4 - 8 * (me // 4), me + 2 - 4 * ((me // 2) % 2)
        near, far = (1 - core) * xs + core * ys, (1 - core) * ys + core * xs

        def remote(src, dst, ss, rs, to):
            return pltpu.make_async_remote_copy(src, dst, ss, rs, device_id={"dp": to}, device_id_type=pl.DeviceIdType.MESH)

        def core_copy(t):
            return remote(send.at[t % 2], recv0.at[t % 3], s0.at[t % 2], r0.at[t % 3], other)

        def near_copy(t):
            return remote(away1.at[t % 2], recv1.at[t % 5], s1.at[t % 2], r1.at[t % 5], near)

        def far_copy(t):
            return remote(away2.at[t % 2], recv2.at[t % 5], s2.at[t % 2], r2.at[t % 5], far)

        def place_of(k, t):
            return got_ref.at[k - 1, :, :, pl.ds(pl.multiple_of(t * FT, FT), FT)]

        def gather_far(t):
            return remote(own_v.at[t], place_of(1, t), s3.at[t], r3.at[t], far)

        def gather_near(t):
            return (remote(own_v.at[t], place_of(2, t), s4.at[t], r4.at[t], near), remote(place_of(1, t), place_of(3, t), s5.at[t], r5.at[t], near))

        def tell(o):
            return remote(sq_ref, all_sq.at[me], s6.at[o - 1], r6.at[me], (me + o) % 8)

        def told(o):
            return remote(sq_ref, all_sq.at[(me + o) % 8], s6.at[o - 1], r6.at[(me + o) % 8], (me + o) % 8)

        def between(first, count):
            return (j >= first) & (j < first + count)

        def behind(steps):
            return between(steps, n) | between(low + steps, n)

        barrier = pltpu.get_barrier_semaphore()

        @pl.when(j == 0)
        def _():
            for o in range(1, 8):
                pl.semaphore_signal(barrier, inc=1, device_id={"dp": (me + o) % 8}, device_id_type=pl.DeviceIdType.MESH)
            for c in copies[:4]:
                c.start()
            sq_ref[...] = jnp.zeros_like(sq_ref)

        @pl.when(between(10, mid))
        def _():
            for c in gather_near(j - 10):
                c.wait()

        @pl.when(between(8, mid))
        def _():
            gather_far(j - 8).wait()

        def finish(out, number):
            t = j - 6
            far_copy(t).wait()
            for i in range(3):
                done = both(stay2[t % 2, i], recv2[t % 5, i])
                out[i] = done
                if number == 0:
                    own_v[t, i] = done
                done = done.astype(F32)
                done = jnp.sum((done * done).reshape(BLK // 8, 8, FT), 0)
                sq_ref[...] += done[:, :128] + done[:, 128:]

        for number, first in enumerate((0, mid, low, low + mid)):

            @pl.when(between(first + 6, mid))
            def _(number=number):
                finish(owns[number], number)

        @pl.when(behind(4))
        def _():
            t = j - 4
            near_copy(t).wait()
            for i in range(3):
                away2[t % 2, i] = both(stay1[t % 2, 1, i], recv1[t % 5, 1, i])
                stay2[t % 2, i] = both(stay1[t % 2, 0, i], recv1[t % 5, 0, i])

        @pl.when(behind(2))
        def _():
            t = j - 2
            core_copy(t).wait()
            for k in range(2):
                for i in range(3):
                    away1[t % 2, k, i] = both(keep[t % 2, 2 + k, i], recv0[t % 3, 2 + k, i])
                    stay1[t % 2, k, i] = both(keep[t % 2, k, i], recv0[t % 3, k, i])

        def tokens(t, upper):
            rows = slice(t * SUB, (t + 1) * SUB)
            if upper:
                g, u = dot(a_v[rows], wg_ref[0]), dot(a_v[rows], wu_ref[0])
            else:
                g, u = g_ref[rows, :], u_ref[rows, :]
            dact = dot_nt(dh_v[rows], wd_ref[0]).astype(BF16).astype(F32)
            s = sigmoid(g)
            gs = g * s
            act_ref[rows, :] = (gs * u).astype(BF16)
            du_ref[rows, :] = (dact * gs).astype(BF16)
            dg_ref[rows, :] = (dact * u * (s + gs * (1.0 - s))).astype(BF16)

        def by_input(t):
            rows = slice(t * SUB, (t + 1) * SUB)
            da = acc[rows, :].astype(BF16).astype(F32)
            wide = a_v[rows, :].astype(F32)
            scale = lax.rsqrt(jnp.mean(wide * wide, -1, keepdims=True) + 1e-6)
            along = jnp.mean(da * wide, -1, keepdims=True) * (scale * scale * scale)
            out = dh_v[rows, :] + (da * scale - wide * along).astype(BF16)
            dh_v[rows, :] = out
            store_turned(me, out, dht_v, rows)

        @pl.when(j == 0)
        def _():
            for c in copies[:2]:
                c.wait()

        @pl.when(j == turn)
        def _():
            copies[5].start()
            copies[4].wait()

        def work(some):
            @pl.when(j < n)
            def _():
                for t in some:
                    tokens(t, True)

            @pl.when(j == turn)
            def _():
                for t in some:
                    by_input(t)

            @pl.when(between(low, n))
            def _():
                for t in some:
                    tokens(t, False)

        work((0,))

        @pl.when(j == 0)
        def _():
            pl.semaphore_wait(barrier, 7)

        @pl.when(j == steps - 1)
        def _():
            for o in range(1, 8):
                tell(o).start()
            all_sq[me] = sq_ref[...]
            for o in range(1, 8):
                tell(o).wait_send()
                told(o).wait_recv()
            total = all_sq[0]
            for d in range(1, 8):
                total = total + all_sq[d]
            total = jnp.sum(jnp.sum(total, 0, keepdims=True), 1, keepdims=True)
            factor = jnp.minimum(1.0, 0.5 * lax.rsqrt(total / (3 * L * D * F) + 1e-30))
            factor_ref[...] = jnp.broadcast_to(factor, (8, 128))

        @pl.when(behind(4))
        def _():
            far_copy(j - 4).start()

        @pl.when(behind(2))
        def _():
            near_copy(j - 2).start()

        @pl.when(behind(1))
        def _():
            core_copy(j - 1).start()

        @pl.when(between(6, mid))
        def _():
            gather_far(j - 6).start()

        @pl.when(between(8, mid))
        def _():
            for c in gather_near(j - 8):
                c.start()

        work(range(1, T // SUB))

        @pl.when(j == n - 1)
        def _():
            copies[4].start()

        @pl.when(j == 0)
        def _():
            for c in copies[2:4]:
                c.wait()

        @pl.when(j == low)
        def _():
            copies[5].wait()

        @pl.when(behind(0))
        def _():
            for i, (left, right) in enumerate(((at_v, dg_ref), (at_v, du_ref), (dht_v, act_ref))):
                for half, out in enumerate((keep, send)):
                    made = dot(left[half * 4 * BLK : (half + 1) * 4 * BLK, :], right[...]).astype(BF16)
                    for k in range(4):
                        out[j % 2, k, i] = made[k * BLK : (k + 1) * BLK]

        def gather_input(first):
            for t in range(T // SUB):
                rows = slice(t * SUB, (t + 1) * SUB)
                more = dot_nt(dg_ref[rows], wg_ref[0]) + dot_nt(du_ref[rows], wu_ref[0])
                acc[rows, :] = more if first else acc[rows, :] + more

        @pl.when(j == 0)
        def _():
            gather_input(True)

        @pl.when(between(1, n - 1))
        def _():
            gather_input(False)

    last = n - 1
    lower = lambda j: jnp.clip(j - low, 0, last)
    whole = pl.BlockSpec(memory_space=pl.ANY)
    weight = pl.BlockSpec((1, D, FT), lambda j: (1, 0, jnp.minimum(j, last)))
    wdown = pl.BlockSpec((1, FT, D), lambda j: (jnp.where(j < n, 1, 0), jnp.where(j < n, j, lower(j)), 0))
    tile = pl.BlockSpec((T, FT), lambda j: (0, lower(j)))

    def shard(first):
        return pl.BlockSpec((3, BLK, FT), lambda j: (0, 0, jnp.clip(j - 6 - first, 0, mid - 1))), shaped((3, BLK, WIDE))

    outs = [shard(first) for first in (0, mid, low, low + mid)]
    outs += [(whole, shaped((3, 3, BLK, WIDE))), (pl.BlockSpec((8, 128), lambda j: (0, 0)), shaped((8, 128), F32))]
    sem = pltpu.SemaphoreType.DMA
    quarter = lambda *lead: pltpu.VMEM((*lead, 3, BLK, FT), BF16)
    scratch = [pltpu.VMEM((T, FT), BF16)] * 3
    scratch += [pltpu.VMEM((T, D), BF16)] * 2 + [pltpu.VMEM((D, T), BF16)] * 2 + [pltpu.VMEM((T, D), F32)]
    scratch += [quarter(2, 4), quarter(2, 4), quarter(3, 4), quarter(2, 2), quarter(2, 2), quarter(5, 2), quarter(2), quarter(2), quarter(5), quarter(mid)]
    scratch += [pltpu.VMEM((8, 128), F32), pltpu.VMEM((8, 8, 128), F32)]
    scratch += [sem((k,)) for k in (6, 2, 3, 2, 5, 2, 5, mid, mid, mid, mid, mid, mid, 7, 8)]
    return pl.pallas_call(
        kernel,
        grid_spec=pltpu.PrefetchScalarGridSpec(
            num_scalar_prefetch=0, grid=(steps,), in_specs=[whole] * 6 + [wdown, weight, weight, tile, tile], out_specs=[s for s, _ in outs], scratch_shapes=scratch
        ),
        out_shape=[o for _, o in outs],
        compiler_params=pltpu.CompilerParams(dimension_semantics=("arbitrary",), vmem_limit_bytes=63 * MB, collective_id=0, has_side_effects=True),
        cost_estimate=pl.CostEstimate(flops=12 * MM, bytes_accessed=120_000_000, transcendentals=0),
        name="backward",
    )(dy, a1, a1t, dyt, h, a0t, w_down, w_gate, w_up, gate, up)


def adamw(me, layer, first, width, base, factor, parts, w, m, v, so_far):
    ft = 640
    steps, at0, part0 = width // ft, first // ft, (first - base) // ft

    def kernel(me_ref, f_ref, *refs):
        parts, refs = refs[:8], refs[8:]
        ws, ms, vs = refs[0:3], refs[3:6], refs[6:9]
        nws, nms, nvs, part = refs[-10:-7], refs[-7:-4], refs[-4:-1], refs[-1]
        f = f_ref[0:1, 0:1]
        p = pl.program_id(0)
        for at in range(8):

            @pl.when(p == at)
            def _(at=at):
                part[...] = parts[at][...]

        def take(i, rows, g):
            g = g.astype(F32) * f
            new_m = 0.9 * ms[i][0, rows, :] + 0.1 * g
            new_v = 0.95 * vs[i][0, rows, :] + 0.05 * g * g
            wide = ws[i][0, rows, :].astype(F32)
            nws[i][0, rows, :] = (wide - 0.02 * (new_m * lax.rsqrt(new_v + 1e-8) + 0.1 * wide)).astype(BF16)
            nms[i][0, rows, :] = new_m
            nvs[i][0, rows, :] = new_v

        for r in range(0, BLK, 16):
            for i in range(2):
                take(i, slice(r, r + 16), part[i, r : r + 16, :])
        for r in range(0, ft, 128):
            take(2, slice(r, r + 128), part[2, :, r : r + 128].T)

    def piece(at):
        where = lambda p, j: part0 + jnp.where(p == at, j, jnp.where(p < at, 0, steps - 1))
        if parts[at][1] is None:
            return pl.BlockSpec((3, BLK, ft), lambda p, j, me_ref: (0, 0, where(p, j)))
        return pl.BlockSpec((None, 3, BLK, ft), lambda p, j, me_ref: (parts[at][1], 0, 0, where(p, j)))

    across = pl.BlockSpec((1, BLK, ft), lambda p, j, me_ref: (layer, shard_at(p, me_ref[0]), at0 + j))
    along = pl.BlockSpec((1, ft, BLK), lambda p, j, me_ref: (layer, at0 + j, shard_at(p, me_ref[0])))
    three = [across, across, along]
    whole = pl.BlockSpec(memory_space=pl.ANY)
    ins = [pl.BlockSpec((8, 128), lambda p, j, me_ref: (0, 0))] + [piece(at) for at in range(8)] + three * 3
    args = [factor] + [a for a, _ in parts] + list(w) + list(m) + list(v)
    outs = [(s, shaped(o.shape, o.dtype)) for s, o in zip(three * 3, list(w) + list(m) + list(v))]
    aliases = {}
    if so_far is not None:
        aliases = {1 + len(ins) + i: i for i in range(9)}
        ins, args = ins + [whole] * 9, args + list(so_far)
    size = 3 * width * D
    return call(kernel, (8, steps), ins, outs, [pltpu.VMEM((3, BLK, ft), BF16)], flops=size * 200, moved=size * 22, aliases=aliases)(me, *args)


CORE = [(i, i ^ 1) for i in range(8)]
FIRST = [(i, i ^ (2 if i & 1 else 4)) for i in range(8)]
SECOND = [(i, i ^ (4 if i & 1 else 2)) for i in range(8)]


STAGES = {"core": CORE, "first": FIRST, "second": SECOND}


def swap(a, stage):
    return lax.ppermute(a, "dp", STAGES[stage])


def gather(own):
    mine = [own, swap(own, "second")]
    mine += [swap(a, "first") for a in mine]
    return [(a, None) for a in mine + [swap(a, "core") for a in mine]]


def solution(mesh):
    def work(x, dy, *arrays):
        weights, m, v = (arrays[i : i + 3] for i in (0, 3, 6))
        w_gate, w_up, w_down = weights
        x, dy = x[0], dy[0]
        me = lax.axis_index("dp").astype(jnp.int32).reshape(1)
        gate, up, act = gate_up(me, x, w_gate, w_up)
        h, a1, a1t, a0t, dyt = down(me, act, w_down, x, dy)
        own1a, own1b, own0a, own0b, got, factor = backward(dy, a1, a1t, dyt, h, a0t, gate, up, *weights)

        parts = [(own1a, None)] + [(got, k) for k in range(3)]
        across = swap(own1a, "core"), swap(got, "core")
        parts += [(across[0], None)] + [(across[1], k) for k in range(3)]
        new = None
        for first in (0, WIDE // 2):
            new = adamw(me, 1, first, WIDE // 2, 0, factor, parts, weights, m, v, new)
        for layer, number, own in ((1, 1, own1b), (0, 0, own0a), (0, 1, own0b)):
            parts = gather(own)
            new = adamw(me, layer, HALVES[number], WIDE, HALVES[number], factor, parts, weights, m, v, new)
        return tuple(new)

    return jax.shard_map(
        work,
        mesh=mesh,
        in_specs=(P(("rep", "dp"), None, None),) * 2 + (P(None, None, None),) * 9,
        out_specs=(P("rep", None, None),) * 9,
        check_vma=False,
    )
```

```python
import jax
import jax.numpy as jnp
from jax import lax
from jax.experimental import pallas as pl
from jax.experimental.pallas import tpu as pltpu
from jax.sharding import PartitionSpec as P


T, D, F, L = 2048, 1024, 2560, 2
FT = 256
BLK = 128
SUB = 512
HALVES = (0, F // 2)
WIDE = F // 2
F32, BF16 = jnp.float32, jnp.bfloat16
MB = 1 << 20

NT = (((1,), (1,)), ((), ()))


def dot(a, b):
    return jnp.dot(a, b, preferred_element_type=F32)


def dot_nt(a, b):
    return lax.dot_general(a, b, NT, preferred_element_type=F32)


def sigmoid(x):
    return 0.5 * jnp.tanh(0.5 * x) + 0.5


def normed(h):
    wide = h.astype(F32)
    scale = lax.rsqrt(jnp.mean(wide * wide, -1, keepdims=True) + 1e-6)
    return (wide * scale).astype(BF16)


def place(shard, me):
    sx, sy, half = (flip + (1 - 2 * flip) * bit for bit, flip in zip((me // 4, (me // 2) % 2, me % 2), (shard >> 2, (shard >> 1) & 1, shard & 1)))
    return half * 4 + (sy * 2 + sx if shard & 1 else sx * 2 + sy)


def shard_at(p, me):
    half, k = p >> 2, p & 3
    hi, lo = k >> 1, k & 1
    core = (me & 1) ^ half
    sx, sy = (1 - core) * hi + core * lo, (1 - core) * lo + core * hi
    return me ^ (sx * 4 + sy * 2 + half)


def store_turned(me, tile, out_ref, columns=slice(None)):
    for shard in range(8):
        rows = pl.ds(pl.multiple_of(place(shard, me) * BLK, BLK), BLK)
        out_ref[rows, columns] = tile[:, shard * BLK : (shard + 1) * BLK].T


def call(kernel, grid, ins, outs, scratch=(), flops=0, moved=0, aliases=None):
    return pl.pallas_call(
        kernel,
        grid_spec=pltpu.PrefetchScalarGridSpec(num_scalar_prefetch=1, grid=grid, in_specs=[s for s in ins], out_specs=[s for s, _ in outs], scratch_shapes=list(scratch)),
        out_shape=[o for _, o in outs],
        compiler_params=pltpu.CompilerParams(dimension_semantics=("arbitrary",) * len(grid), vmem_limit_bytes=63 * MB),
        cost_estimate=pl.CostEstimate(flops=int(flops), bytes_accessed=int(moved), transcendentals=0),
        input_output_aliases=aliases or {},
    )


def shaped(shape, dtype=BF16):
    return jax.ShapeDtypeStruct(shape, dtype)


MM = 2 * T * D * F


def forward(me, x, dy, w_gate, w_up, w_down):
    n, rows = F // FT, T // 8

    def kernel(me_ref, x_ref, dy_ref, wg_ref, wu_ref, wd_ref, g_ref, u_ref, out_ref, a1_ref, a1t_ref, a0t_ref, dyt_ref, a_ref, acc_ref):
        j = pl.program_id(0)

        @pl.when(j == 0)
        def _():
            for t in range(T // SUB):
                here = slice(t * SUB, (t + 1) * SUB)
                a_ref[here, :] = normed(x_ref[here, :])

        def tile(first):
            for t in range(T // SUB):
                here = slice(t * SUB, (t + 1) * SUB)
                g = dot(a_ref[here], wg_ref[0])
                u = dot(a_ref[here], wu_ref[0])
                g_ref[here, :] = g
                u_ref[here, :] = u
                more = dot((g * sigmoid(g) * u).astype(BF16), wd_ref[0])
                acc_ref[here, :] = more if first else acc_ref[here, :] + more
            chunk = pl.ds(pl.multiple_of(jnp.minimum(j, 7) * rows, rows), rows)
            store_turned(me_ref[0], a_ref[chunk, :], a0t_ref)
            store_turned(me_ref[0], dy_ref[...], dyt_ref)

        @pl.when(j == 0)
        def _():
            tile(True)

        @pl.when((j > 0) & (j < n))
        def _():
            tile(False)

        @pl.when(j >= n)
        def _():
            here = pl.ds(pl.multiple_of((j - n) * SUB, SUB), SUB)
            out = x_ref[here, :] + acc_ref[here, :].astype(BF16)
            out_ref[...] = out
            a = normed(out)
            a1_ref[...] = a
            store_turned(me_ref[0], a, a1t_ref)

    tile = lambda j: jnp.minimum(j, n - 1)
    row = lambda j: jnp.maximum(j - n, 0)
    part = lambda j: jnp.minimum(j, 7)
    weight = pl.BlockSpec((1, D, FT), lambda j, m: (0, 0, tile(j)))
    kept = pl.BlockSpec((T, FT), lambda j, m: (0, tile(j)))
    tall = pl.BlockSpec((SUB, D), lambda j, m: (row(j), 0))
    flat = pl.BlockSpec((D, rows), lambda j, m: (0, part(j)))
    return call(
        kernel,
        (n + T // SUB,),
        [
            pl.BlockSpec((T, D), lambda j, m: (0, 0), pipeline_mode=pl.Buffered(1)),
            pl.BlockSpec((rows, D), lambda j, m: (part(j), 0)),
            weight,
            weight,
            pl.BlockSpec((1, FT, D), lambda j, m: (0, tile(j), 0)),
        ],
        [(kept, shaped((T, F), F32))] * 2
        + [(tall, shaped((T, D)))] * 2
        + [(pl.BlockSpec((D, SUB), lambda j, m: (0, row(j))), shaped((D, T))), (flat, shaped((D, T))), (flat, shaped((D, T)))],
        [pltpu.VMEM((T, D), BF16), pltpu.VMEM((T, D), F32)],
        flops=3 * MM,
        moved=90e6,
    )(me, x, dy, w_gate, w_up, w_down)


def both(a, b):
    return (a.astype(F32) + b.astype(F32)).astype(BF16)


def backward(dy, a1, a1t, dyt, h, a0t, gate, up, w_gate, w_up, w_down):
    n = F // FT
    mid = n // 2
    turn, low = n, n + 1
    end = low + n
    steps = end + 7

    def kernel(*refs):
        refs = list(refs)
        take = lambda count: [refs.pop(0) for _ in range(count)]
        dy_ref, a1_ref, a1t_ref, dyt_ref, h_ref, a0t_ref = take(6)
        wd_ref, wg_ref, wu_ref, g_ref, u_ref = take(5)
        owns = take(4)
        got_ref, over_ref, factor_ref = take(3)
        dg_ref, du_ref, act_ref = take(3)
        dh_v, a_v, at_v, dht_v, acc = take(5)
        keep, send, recv0, away1, stay1, recv1, away2, stay2, recv2, own_v = take(10)
        sq_ref, all_sq = take(2)
        sems, s0, r0, s1, r1, s2, r2, s3, r3, s4, r4, s5, r5, s6, r6, s7, r7 = take(17)
        pairs = ((dy_ref, dh_v), (a1_ref, a_v), (a1t_ref, at_v), (dyt_ref, dht_v), (h_ref, a_v), (a0t_ref, at_v))
        copies = [pltpu.make_async_copy(s, d, sems.at[i]) for i, (s, d) in enumerate(pairs)]
        j = pl.program_id(0)
        me = lax.axis_index("dp")
        core = me % 2
        other = me + 1 - 2 * core
        xs, ys = me + 4 - 8 * (me // 4), me + 2 - 4 * ((me // 2) % 2)
        near, far = (1 - core) * xs + core * ys, (1 - core) * ys + core * xs

        def remote(src, dst, ss, rs, to):
            return pltpu.make_async_remote_copy(src, dst, ss, rs, device_id={"dp": to}, device_id_type=pl.DeviceIdType.MESH)

        def core_copy(t):
            return remote(send.at[t % 2], recv0.at[t % 3], s0.at[t % 2], r0.at[t % 3], other)

        def near_copy(t):
            return remote(away1.at[t % 2], recv1.at[t % 5], s1.at[t % 2], r1.at[t % 5], near)

        def far_copy(t):
            return remote(away2.at[t % 2], recv2.at[t % 5], s2.at[t % 2], r2.at[t % 5], far)

        def place_of(k, t):
            return got_ref.at[k - 1, :, :, pl.ds(pl.multiple_of(t * FT, FT), FT)]

        def gather_far(t):
            return remote(own_v.at[t], place_of(1, t), s3.at[t], r3.at[t], far)

        def gather_near(t):
            return (remote(own_v.at[t], place_of(2, t), s4.at[t], r4.at[t], near), remote(place_of(1, t), place_of(3, t), s5.at[t], r5.at[t], near))

        def core_swaps():
            tiles = [remote(own_v.at[t], over_ref.at[0, :, :, pl.ds(t * FT, FT)], s7.at[t], r7.at[t], other) for t in range(mid)]
            return tiles + [remote(got_ref, over_ref.at[pl.ds(1, 3)], s7.at[mid], r7.at[mid], other)]

        def tell(o):
            return remote(sq_ref, all_sq.at[me], s6.at[o - 1], r6.at[me], (me + o) % 8)

        def told(o):
            return remote(sq_ref, all_sq.at[(me + o) % 8], s6.at[o - 1], r6.at[(me + o) % 8], (me + o) % 8)

        def between(first, count):
            return (j >= first) & (j < first + count)

        def behind(steps):
            return between(steps, n) | between(low + steps, n)

        def two_speeds(steps, slower, work):
            @pl.when(between(steps, n))
            def _():
                work(j - steps)

            @pl.when(between(low + slower, n))
            def _():
                work(j - slower)

        barrier = pltpu.get_barrier_semaphore()

        @pl.when(j == 0)
        def _():
            for o in range(1, 8):
                pl.semaphore_signal(barrier, inc=1, device_id={"dp": (me + o) % 8}, device_id_type=pl.DeviceIdType.MESH)
            for c in copies[:4]:
                c.start()
            sq_ref[...] = jnp.zeros_like(sq_ref)

        @pl.when(between(8, mid))
        def _():
            for c in gather_near(j - 8):
                c.wait()

        @pl.when(between(6, mid))
        def _():
            gather_far(j - 6).wait()

        @pl.when(j == 16)
        def _():
            for c in core_swaps():
                c.wait()

        def finish(out, number):
            t = j - (4 if number < 2 else 6)
            far_copy(t).wait()
            for i in range(3):
                done = both(stay2[t % 2, i], recv2[t % 5, i])
                out[i] = done
                if number == 0:
                    own_v[t, i] = done
                done = done.astype(F32)
                done = jnp.sum((done * done).reshape(BLK // 8, 8, FT), 0)
                sq_ref[...] += done[:, :128] + done[:, 128:]

        for number, first in enumerate((0, mid, low, low + mid)):

            @pl.when(between(first + (4 if number < 2 else 6), mid))
            def _(number=number):
                finish(owns[number], number)

        def second_sum(t):
            near_copy(t).wait()
            for i in range(3):
                away2[t % 2, i] = both(stay1[t % 2, 1, i], recv1[t % 5, 1, i])
                stay2[t % 2, i] = both(stay1[t % 2, 0, i], recv1[t % 5, 0, i])

        two_speeds(3, 4, second_sum)

        @pl.when(behind(2))
        def _():
            t = j - 2
            core_copy(t).wait()
            for k in range(2):
                for i in range(3):
                    away1[t % 2, k, i] = both(keep[t % 2, 2 + k, i], recv0[t % 3, 2 + k, i])
                    stay1[t % 2, k, i] = both(keep[t % 2, k, i], recv0[t % 3, k, i])

        def tokens(t, upper):
            rows = slice(t * SUB, (t + 1) * SUB)
            if upper:
                g, u = dot(a_v[rows], wg_ref[0]), dot(a_v[rows], wu_ref[0])
            else:
                g, u = g_ref[rows, :], u_ref[rows, :]
            dact = dot_nt(dh_v[rows], wd_ref[0]).astype(BF16).astype(F32)
            s = sigmoid(g)
            gs = g * s
            act_ref[rows, :] = (gs * u).astype(BF16)
            du_ref[rows, :] = (dact * gs).astype(BF16)
            dg_ref[rows, :] = (dact * u * (s + gs * (1.0 - s))).astype(BF16)

        def by_input(t):
            rows = slice(t * SUB, (t + 1) * SUB)
            da = acc[rows, :].astype(BF16).astype(F32)
            wide = a_v[rows, :].astype(F32)
            scale = lax.rsqrt(jnp.mean(wide * wide, -1, keepdims=True) + 1e-6)
            along = jnp.mean(da * wide, -1, keepdims=True) * (scale * scale * scale)
            out = dh_v[rows, :] + (da * scale - wide * along).astype(BF16)
            dh_v[rows, :] = out
            store_turned(me, out, dht_v, rows)

        @pl.when(j == 0)
        def _():
            for c in copies[:2]:
                c.wait()

        @pl.when(j == turn)
        def _():
            copies[5].start()
            copies[4].wait()

        def work(some):
            @pl.when(j < n)
            def _():
                for t in some:
                    tokens(t, True)

            @pl.when(j == turn)
            def _():
                for t in some:
                    by_input(t)

            @pl.when(between(low, n))
            def _():
                for t in some:
                    tokens(t, False)

        work((0,))

        @pl.when(j == 0)
        def _():
            pl.semaphore_wait(barrier, 7)

        @pl.when(j == steps - 1)
        def _():
            for o in range(1, 8):
                tell(o).start()
            all_sq[me] = sq_ref[...]
            for o in range(1, 8):
                tell(o).wait_send()
                told(o).wait_recv()
            total = all_sq[0]
            for d in range(1, 8):
                total = total + all_sq[d]
            total = jnp.sum(jnp.sum(total, 0, keepdims=True), 1, keepdims=True)
            factor = jnp.minimum(1.0, 0.5 * lax.rsqrt(total / (3 * L * D * F) + 1e-30))
            factor_ref[...] = jnp.broadcast_to(factor, (8, 128))

        two_speeds(3, 4, lambda t: far_copy(t).start())

        @pl.when(behind(2))
        def _():
            near_copy(j - 2).start()

        @pl.when(behind(1))
        def _():
            core_copy(j - 1).start()

        @pl.when(between(4, mid))
        def _():
            gather_far(j - 4).start()

        @pl.when(j == 13)
        def _():
            for c in core_swaps():
                c.start()

        @pl.when(between(6, mid))
        def _():
            for c in gather_near(j - 6):
                c.start()

        work(range(1, T // SUB))

        @pl.when(j == n - 1)
        def _():
            copies[4].start()

        @pl.when(j == 0)
        def _():
            for c in copies[2:4]:
                c.wait()

        @pl.when(j == low)
        def _():
            copies[5].wait()

        @pl.when(behind(0))
        def _():
            for i, (left, right) in enumerate(((at_v, dg_ref), (at_v, du_ref), (dht_v, act_ref))):
                for half, out in enumerate((keep, send)):
                    made = dot(left[half * 4 * BLK : (half + 1) * 4 * BLK, :], right[...]).astype(BF16)
                    for k in range(4):
                        out[j % 2, k, i] = made[k * BLK : (k + 1) * BLK]

        def gather_input(first):
            for t in range(T // SUB):
                rows = slice(t * SUB, (t + 1) * SUB)
                more = dot_nt(dg_ref[rows], wg_ref[0]) + dot_nt(du_ref[rows], wu_ref[0])
                acc[rows, :] = more if first else acc[rows, :] + more

        @pl.when(j == 0)
        def _():
            gather_input(True)

        @pl.when(between(1, n - 1))
        def _():
            gather_input(False)

    last = n - 1
    lower = lambda j: jnp.clip(j - low, 0, last)
    whole = pl.BlockSpec(memory_space=pl.ANY)
    weight = pl.BlockSpec((1, D, FT), lambda j: (1, 0, jnp.minimum(j, last)))
    wdown = pl.BlockSpec((1, FT, D), lambda j: (jnp.where(j < n, 1, 0), jnp.where(j < n, j, lower(j)), 0))
    tile = pl.BlockSpec((T, FT), lambda j: (0, lower(j)))

    def shard(first):
        return pl.BlockSpec((3, BLK, FT), lambda j: (0, 0, jnp.clip(j - first, 0, mid - 1))), shaped((3, BLK, WIDE))

    outs = [shard(first) for first in (4, 4 + mid, low + 6, low + 6 + mid)]
    outs += [(whole, shaped((3, 3, BLK, WIDE))), (whole, shaped((4, 3, BLK, WIDE))), (pl.BlockSpec((8, 128), lambda j: (0, 0)), shaped((8, 128), F32))]
    sem = pltpu.SemaphoreType.DMA
    quarter = lambda *lead: pltpu.VMEM((*lead, 3, BLK, FT), BF16)
    scratch = [pltpu.VMEM((T, FT), BF16)] * 3
    scratch += [pltpu.VMEM((T, D), BF16)] * 2 + [pltpu.VMEM((D, T), BF16)] * 2 + [pltpu.VMEM((T, D), F32)]
    scratch += [quarter(2, 4), quarter(2, 4), quarter(3, 4), quarter(2, 2), quarter(2, 2), quarter(5, 2), quarter(2), quarter(2), quarter(5), quarter(mid)]
    scratch += [pltpu.VMEM((8, 128), F32), pltpu.VMEM((8, 8, 128), F32)]
    scratch += [sem((k,)) for k in (6, 2, 3, 2, 5, 2, 5, mid, mid, mid, mid, mid, mid, 7, 8, mid + 1, mid + 1)]
    return pl.pallas_call(
        kernel,
        grid_spec=pltpu.PrefetchScalarGridSpec(
            num_scalar_prefetch=0, grid=(steps,), in_specs=[whole] * 6 + [wdown, weight, weight, tile, tile], out_specs=[s for s, _ in outs], scratch_shapes=scratch
        ),
        out_shape=[o for _, o in outs],
        compiler_params=pltpu.CompilerParams(dimension_semantics=("arbitrary",), vmem_limit_bytes=63 * MB, collective_id=0, has_side_effects=True),
        cost_estimate=pl.CostEstimate(flops=12 * MM, bytes_accessed=120_000_000, transcendentals=0),
        name="backward",
    )(dy, a1, a1t, dyt, h, a0t, w_down, w_gate, w_up, gate, up)


def adamw(me, layer, first, width, base, factor, parts, w, m, v, so_far):
    ft = width
    steps, at0, part0 = width // ft, first // ft, (first - base) // ft

    def kernel(me_ref, f_ref, *refs):
        parts, refs = refs[:8], refs[8:]
        ws, ms, vs = refs[0:3], refs[3:6], refs[6:9]
        nws, nms, nvs, part = refs[-10:-7], refs[-7:-4], refs[-4:-1], refs[-1]
        f = f_ref[0:1, 0:1]
        p = pl.program_id(0)
        for at in range(8):

            @pl.when(p == at)
            def _(at=at):
                part[...] = parts[at][...]

        def take(i, rows, g):
            g = g.astype(F32) * f
            new_m = 0.9 * ms[i][0, rows, :] + 0.1 * g
            new_v = 0.95 * vs[i][0, rows, :] + 0.05 * g * g
            wide = ws[i][0, rows, :].astype(F32)
            nws[i][0, rows, :] = (wide - 0.02 * (new_m * lax.rsqrt(new_v + 1e-8) + 0.1 * wide)).astype(BF16)
            nms[i][0, rows, :] = new_m
            nvs[i][0, rows, :] = new_v

        for r in range(0, BLK, 16):
            for i in range(2):
                take(i, slice(r, r + 16), part[i, r : r + 16, :])
        for r in range(0, ft, 128):
            take(2, slice(r, r + 128), part[2, :, r : r + 128].T)

    def piece(at):
        where = lambda p, j: part0 + jnp.where(p == at, j, jnp.where(p < at, 0, steps - 1))
        if parts[at][1] is None:
            return pl.BlockSpec((3, BLK, ft), lambda p, j, me_ref: (0, 0, where(p, j)))
        return pl.BlockSpec((None, 3, BLK, ft), lambda p, j, me_ref: (parts[at][1], 0, 0, where(p, j)))

    across = pl.BlockSpec((1, BLK, ft), lambda p, j, me_ref: (layer, shard_at(p, me_ref[0]), at0 + j))
    along = pl.BlockSpec((1, ft, BLK), lambda p, j, me_ref: (layer, at0 + j, shard_at(p, me_ref[0])))
    three = [across, across, along]
    whole = pl.BlockSpec(memory_space=pl.ANY)
    ins = [pl.BlockSpec((8, 128), lambda p, j, me_ref: (0, 0))] + [piece(at) for at in range(8)] + three * 3
    args = [factor] + [a for a, _ in parts] + list(w) + list(m) + list(v)
    outs = [(s, shaped(o.shape, o.dtype)) for s, o in zip(three * 3, list(w) + list(m) + list(v))]
    aliases = {}
    if so_far is not None:
        aliases = {1 + len(ins) + i: i for i in range(9)}
        ins, args = ins + [whole] * 9, args + list(so_far)
    size = 3 * width * D
    return call(kernel, (8, steps), ins, outs, [pltpu.VMEM((3, BLK, ft), BF16)], flops=size * 200, moved=size * 22, aliases=aliases)(me, *args)


CORE = [(i, i ^ 1) for i in range(8)]
FIRST = [(i, i ^ (2 if i & 1 else 4)) for i in range(8)]
SECOND = [(i, i ^ (4 if i & 1 else 2)) for i in range(8)]


STAGES = {"core": CORE, "first": FIRST, "second": SECOND}


def swap(a, stage):
    return lax.ppermute(a, "dp", STAGES[stage])


def gather(own):
    mine = [own, swap(own, "second")]
    mine += [swap(a, "first") for a in mine]
    return [(a, None) for a in mine + [swap(a, "core") for a in mine]]


def solution(mesh):
    def work(x, dy, *arrays):
        weights, m, v = (arrays[i : i + 3] for i in (0, 3, 6))
        w_gate, w_up, w_down = weights
        x, dy = x[0], dy[0]
        me = lax.axis_index("dp").astype(jnp.int32).reshape(1)
        gate, up, h, a1, a1t, a0t, dyt = forward(me, x, dy, *weights)
        own1a, own1b, own0a, own0b, got, over, factor = backward(dy, a1, a1t, dyt, h, a0t, gate, up, *weights)

        parts = [(own1a, None)] + [(got, k) for k in range(3)] + [(over, k) for k in range(4)]
        new = None
        for first in (0, WIDE // 2):
            new = adamw(me, 1, first, WIDE // 2, 0, factor, parts, weights, m, v, new)
        for layer, number, own in ((1, 1, own1b), (0, 0, own0a), (0, 1, own0b)):
            parts = gather(own)
            new = adamw(me, layer, HALVES[number], WIDE, HALVES[number], factor, parts, weights, m, v, new)
        return tuple(new)

    return jax.shard_map(
        work,
        mesh=mesh,
        in_specs=(P(("rep", "dp"), None, None),) * 2 + (P(None, None, None),) * 9,
        out_specs=(P("rep", None, None),) * 9,
        check_vma=False,
    )
```

```python
import jax
import jax.numpy as jnp
from jax import lax
from jax.experimental import pallas as pl
from jax.experimental.pallas import tpu as pltpu
from jax.sharding import PartitionSpec as P


T, D, F, L = 2048, 1024, 2560, 2
FT = 256
BLK = 128
SUB = 512
HALVES = (0, F // 2)
WIDE = F // 2
F32, BF16 = jnp.float32, jnp.bfloat16
MB = 1 << 20

NT = (((1,), (1,)), ((), ()))


def dot(a, b):
    return jnp.dot(a, b, preferred_element_type=F32)


def dot_nt(a, b):
    return lax.dot_general(a, b, NT, preferred_element_type=F32)


def sigmoid(x):
    return 0.5 * jnp.tanh(0.5 * x) + 0.5


def normed(h):
    wide = h.astype(F32)
    scale = lax.rsqrt(jnp.mean(wide * wide, -1, keepdims=True) + 1e-6)
    return (wide * scale).astype(BF16)


def place(shard, me):
    sx, sy, half = (flip + (1 - 2 * flip) * bit for bit, flip in zip((me // 4, (me // 2) % 2, me % 2), (shard >> 2, (shard >> 1) & 1, shard & 1)))
    return half * 4 + (sy * 2 + sx if shard & 1 else sx * 2 + sy)


def shard_at(p, me):
    half, k = p >> 2, p & 3
    hi, lo = k >> 1, k & 1
    core = (me & 1) ^ half
    sx, sy = (1 - core) * hi + core * lo, (1 - core) * lo + core * hi
    return me ^ (sx * 4 + sy * 2 + half)


def store_turned(me, tile, out_ref, columns=slice(None)):
    for shard in range(8):
        rows = pl.ds(pl.multiple_of(place(shard, me) * BLK, BLK), BLK)
        out_ref[rows, columns] = tile[:, shard * BLK : (shard + 1) * BLK].T


def call(kernel, grid, ins, outs, scratch=(), flops=0, moved=0, aliases=None):
    return pl.pallas_call(
        kernel,
        grid_spec=pltpu.PrefetchScalarGridSpec(num_scalar_prefetch=1, grid=grid, in_specs=[s for s in ins], out_specs=[s for s, _ in outs], scratch_shapes=list(scratch)),
        out_shape=[o for _, o in outs],
        compiler_params=pltpu.CompilerParams(dimension_semantics=("arbitrary",) * len(grid), vmem_limit_bytes=63 * MB),
        cost_estimate=pl.CostEstimate(flops=int(flops), bytes_accessed=int(moved), transcendentals=0),
        input_output_aliases=aliases or {},
    )


def shaped(shape, dtype=BF16):
    return jax.ShapeDtypeStruct(shape, dtype)


MM = 2 * T * D * F


def forward(me, x, dy, w_gate, w_up, w_down):
    n, rows = F // FT, T // 8

    def kernel(me_ref, x_ref, dy_ref, wg_ref, wu_ref, wd_ref, g_ref, u_ref, out_ref, a1_ref, a1t_ref, a0t_ref, dyt_ref, a_ref, acc_ref):
        j = pl.program_id(0)

        @pl.when(j == 0)
        def _():
            for t in range(T // SUB):
                here = slice(t * SUB, (t + 1) * SUB)
                a_ref[here, :] = normed(x_ref[here, :])

        def tile(first):
            for t in range(T // SUB):
                here = slice(t * SUB, (t + 1) * SUB)
                g = dot(a_ref[here], wg_ref[0])
                u = dot(a_ref[here], wu_ref[0])
                g_ref[here, :] = g
                u_ref[here, :] = u
                more = dot((g * sigmoid(g) * u).astype(BF16), wd_ref[0])
                acc_ref[here, :] = more if first else acc_ref[here, :] + more
            chunk = pl.ds(pl.multiple_of(jnp.minimum(j, 7) * rows, rows), rows)
            store_turned(me_ref[0], a_ref[chunk, :], a0t_ref)
            store_turned(me_ref[0], dy_ref[...], dyt_ref)

        @pl.when(j == 0)
        def _():
            tile(True)

        @pl.when((j > 0) & (j < n))
        def _():
            tile(False)

        @pl.when(j >= n)
        def _():
            here = pl.ds(pl.multiple_of((j - n) * SUB, SUB), SUB)
            out = x_ref[here, :] + acc_ref[here, :].astype(BF16)
            out_ref[...] = out
            a = normed(out)
            a1_ref[...] = a
            store_turned(me_ref[0], a, a1t_ref)

    tile = lambda j: jnp.minimum(j, n - 1)
    row = lambda j: jnp.maximum(j - n, 0)
    part = lambda j: jnp.minimum(j, 7)
    weight = pl.BlockSpec((1, D, FT), lambda j, m: (0, 0, tile(j)))
    kept = pl.BlockSpec((T, FT), lambda j, m: (0, tile(j)))
    tall = pl.BlockSpec((SUB, D), lambda j, m: (row(j), 0))
    flat = pl.BlockSpec((D, rows), lambda j, m: (0, part(j)))
    return call(
        kernel,
        (n + T // SUB,),
        [
            pl.BlockSpec((T, D), lambda j, m: (0, 0), pipeline_mode=pl.Buffered(1)),
            pl.BlockSpec((rows, D), lambda j, m: (part(j), 0)),
            weight,
            weight,
            pl.BlockSpec((1, FT, D), lambda j, m: (0, tile(j), 0)),
        ],
        [(kept, shaped((T, F), F32))] * 2
        + [(tall, shaped((T, D)))] * 2
        + [(pl.BlockSpec((D, SUB), lambda j, m: (0, row(j))), shaped((D, T))), (flat, shaped((D, T))), (flat, shaped((D, T)))],
        [pltpu.VMEM((T, D), BF16), pltpu.VMEM((T, D), F32)],
        flops=3 * MM,
        moved=90e6,
    )(me, x, dy, w_gate, w_up, w_down)


def both(a, b):
    return (a.astype(F32) + b.astype(F32)).astype(BF16)


def backward(dy, a1, a1t, dyt, h, a0t, gate, up, w_gate, w_up, w_down):
    n = F // FT
    mid = n // 2
    turn, low = n, n + 1
    end = low + n
    steps = end + 6

    def kernel(*refs):
        refs = list(refs)
        take = lambda count: [refs.pop(0) for _ in range(count)]
        dy_ref, a1_ref, a1t_ref, dyt_ref, h_ref, a0t_ref = take(6)
        wd_ref, wg_ref, wu_ref, g_ref, u_ref = take(5)
        owns = take(4)
        got_ref, over_ref, factor_ref = take(3)
        dg_ref, du_ref, act_ref = take(3)
        dh_v, a_v, at_v, dht_v, acc = take(5)
        keep, send, recv0, away1, stay1, recv1, away2, stay2, recv2, own_v = take(10)
        sq_ref, all_sq = take(2)
        sems, s0, r0, s1, r1, s2, r2, s3, r3, s4, r4, s5, r5, s6, r6, s7, r7 = take(17)
        pairs = ((dy_ref, dh_v), (a1_ref, a_v), (a1t_ref, at_v), (dyt_ref, dht_v), (h_ref, a_v), (a0t_ref, at_v))
        copies = [pltpu.make_async_copy(s, d, sems.at[i]) for i, (s, d) in enumerate(pairs)]
        j = pl.program_id(0)
        me = lax.axis_index("dp")
        core = me % 2
        other = me + 1 - 2 * core
        xs, ys = me + 4 - 8 * (me // 4), me + 2 - 4 * ((me // 2) % 2)
        near, far = (1 - core) * xs + core * ys, (1 - core) * ys + core * xs

        def remote(src, dst, ss, rs, to):
            return pltpu.make_async_remote_copy(src, dst, ss, rs, device_id={"dp": to}, device_id_type=pl.DeviceIdType.MESH)

        def core_copy(t):
            return remote(send.at[t % 2], recv0.at[t % 3], s0.at[t % 2], r0.at[t % 3], other)

        def near_copy(t):
            return remote(away1.at[t % 2], recv1.at[t % 5], s1.at[t % 2], r1.at[t % 5], near)

        def far_copy(t):
            return remote(away2.at[t % 2], recv2.at[t % 5], s2.at[t % 2], r2.at[t % 5], far)

        def place_of(k, t):
            return got_ref.at[k - 1, :, :, pl.ds(pl.multiple_of(t * FT, FT), FT)]

        def gather_far(t):
            return remote(own_v.at[t], place_of(1, t), s3.at[t], r3.at[t], far)

        def gather_near(t):
            return (remote(own_v.at[t], place_of(2, t), s4.at[t], r4.at[t], near), remote(place_of(1, t), place_of(3, t), s5.at[t], r5.at[t], near))

        def core_swaps():
            tiles = [remote(own_v.at[t], over_ref.at[0, :, :, pl.ds(t * FT, FT)], s7.at[t], r7.at[t], other) for t in range(mid)]
            return tiles + [remote(got_ref, over_ref.at[pl.ds(1, 3)], s7.at[mid], r7.at[mid], other)]

        def tell(o):
            return remote(sq_ref, all_sq.at[me], s6.at[o - 1], r6.at[me], (me + o) % 8)

        def told(o):
            return remote(sq_ref, all_sq.at[(me + o) % 8], s6.at[o - 1], r6.at[(me + o) % 8], (me + o) % 8)

        def between(first, count):
            return (j >= first) & (j < first + count)

        def behind(steps):
            return between(steps, n) | between(low + steps, n)

        def two_speeds(steps, slower, work):
            @pl.when(between(steps, n))
            def _():
                work(j - steps)

            @pl.when(between(low + slower, n))
            def _():
                work(j - slower)

        barrier = pltpu.get_barrier_semaphore()

        @pl.when(j == 0)
        def _():
            for o in range(1, 8):
                pl.semaphore_signal(barrier, inc=1, device_id={"dp": (me + o) % 8}, device_id_type=pl.DeviceIdType.MESH)
            for c in copies[:4]:
                c.start()
            sq_ref[...] = jnp.zeros_like(sq_ref)

        @pl.when(between(8, mid))
        def _():
            for c in gather_near(j - 8):
                c.wait()

        @pl.when(between(6, mid))
        def _():
            gather_far(j - 6).wait()

        @pl.when(j == 16)
        def _():
            for c in core_swaps():
                c.wait()

        def finish(out, number):
            t = j - (4 if number < 2 else 5)
            far_copy(t).wait()
            for i in range(3):
                done = both(stay2[t % 2, i], recv2[t % 5, i])
                out[i] = done
                if number == 0:
                    own_v[t, i] = done
                done = done.astype(F32)
                done = jnp.sum((done * done).reshape(BLK // 8, 8, FT), 0)
                sq_ref[...] += done[:, :128] + done[:, 128:]

        for number, first in enumerate((0, mid, low, low + mid)):

            @pl.when(between(first + (4 if number < 2 else 5), mid))
            def _(number=number):
                finish(owns[number], number)

        def second_sum(t):
            near_copy(t).wait()
            for i in range(3):
                away2[t % 2, i] = both(stay1[t % 2, 1, i], recv1[t % 5, 1, i])
                stay2[t % 2, i] = both(stay1[t % 2, 0, i], recv1[t % 5, 0, i])

        two_speeds(3, 4, second_sum)

        @pl.when(behind(2))
        def _():
            t = j - 2
            core_copy(t).wait()
            for k in range(2):
                for i in range(3):
                    away1[t % 2, k, i] = both(keep[t % 2, 2 + k, i], recv0[t % 3, 2 + k, i])
                    stay1[t % 2, k, i] = both(keep[t % 2, k, i], recv0[t % 3, k, i])

        def tokens(t, upper):
            rows = slice(t * SUB, (t + 1) * SUB)
            if upper:
                g, u = dot(a_v[rows], wg_ref[0]), dot(a_v[rows], wu_ref[0])
            else:
                g, u = g_ref[rows, :], u_ref[rows, :]
            dact = dot_nt(dh_v[rows], wd_ref[0]).astype(BF16).astype(F32)
            s = sigmoid(g)
            gs = g * s
            act_ref[rows, :] = (gs * u).astype(BF16)
            du_ref[rows, :] = (dact * gs).astype(BF16)
            dg_ref[rows, :] = (dact * u * (s + gs * (1.0 - s))).astype(BF16)

        def by_input(t):
            rows = slice(t * SUB, (t + 1) * SUB)
            da = acc[rows, :].astype(BF16).astype(F32)
            wide = a_v[rows, :].astype(F32)
            scale = lax.rsqrt(jnp.mean(wide * wide, -1, keepdims=True) + 1e-6)
            along = jnp.mean(da * wide, -1, keepdims=True) * (scale * scale * scale)
            out = dh_v[rows, :] + (da * scale - wide * along).astype(BF16)
            dh_v[rows, :] = out
            store_turned(me, out, dht_v, rows)

        @pl.when(j == 0)
        def _():
            for c in copies[:2]:
                c.wait()

        @pl.when(j == turn)
        def _():
            copies[5].start()
            copies[4].wait()

        def work(some):
            @pl.when(j < n)
            def _():
                for t in some:
                    tokens(t, True)

            @pl.when(j == turn)
            def _():
                for t in some:
                    by_input(t)

            @pl.when(between(low, n))
            def _():
                for t in some:
                    tokens(t, False)

        work((0,))

        @pl.when(j == 0)
        def _():
            pl.semaphore_wait(barrier, 7)

        @pl.when(j == steps - 1)
        def _():
            for o in range(1, 8):
                tell(o).start()
            all_sq[me] = sq_ref[...]
            for o in range(1, 8):
                tell(o).wait_send()
                told(o).wait_recv()
            total = all_sq[0]
            for d in range(1, 8):
                total = total + all_sq[d]
            total = jnp.sum(jnp.sum(total, 0, keepdims=True), 1, keepdims=True)
            factor = jnp.minimum(1.0, 0.5 * lax.rsqrt(total / (3 * L * D * F) + 1e-30))
            factor_ref[...] = jnp.broadcast_to(factor, (8, 128))

        two_speeds(3, 4, lambda t: far_copy(t).start())

        @pl.when(behind(2))
        def _():
            near_copy(j - 2).start()

        @pl.when(behind(1))
        def _():
            core_copy(j - 1).start()

        @pl.when(between(4, mid))
        def _():
            gather_far(j - 4).start()

        @pl.when(j == 13)
        def _():
            for c in core_swaps():
                c.start()

        @pl.when(between(6, mid))
        def _():
            for c in gather_near(j - 6):
                c.start()

        work(range(1, T // SUB))

        @pl.when(j == n - 1)
        def _():
            copies[4].start()

        @pl.when(j == 0)
        def _():
            for c in copies[2:4]:
                c.wait()

        @pl.when(j == low)
        def _():
            copies[5].wait()

        @pl.when(behind(0))
        def _():
            for i, (left, right) in enumerate(((at_v, dg_ref), (at_v, du_ref), (dht_v, act_ref))):
                for half, out in enumerate((keep, send)):
                    made = dot(left[half * 4 * BLK : (half + 1) * 4 * BLK, :], right[...]).astype(BF16)
                    for k in range(4):
                        out[j % 2, k, i] = made[k * BLK : (k + 1) * BLK]

        def gather_input(first):
            for t in range(T // SUB):
                rows = slice(t * SUB, (t + 1) * SUB)
                more = dot_nt(dg_ref[rows], wg_ref[0]) + dot_nt(du_ref[rows], wu_ref[0])
                acc[rows, :] = more if first else acc[rows, :] + more

        @pl.when(j == 0)
        def _():
            gather_input(True)

        @pl.when(between(1, n - 1))
        def _():
            gather_input(False)

    last = n - 1
    lower = lambda j: jnp.clip(j - low, 0, last)
    whole = pl.BlockSpec(memory_space=pl.ANY)
    weight = pl.BlockSpec((1, D, FT), lambda j: (1, 0, jnp.minimum(j, last)))
    wdown = pl.BlockSpec((1, FT, D), lambda j: (jnp.where(j < n, 1, 0), jnp.where(j < n, j, lower(j)), 0))
    tile = pl.BlockSpec((T, FT), lambda j: (0, lower(j)))

    def shard(first):
        return pl.BlockSpec((3, BLK, FT), lambda j: (0, 0, jnp.clip(j - first, 0, mid - 1))), shaped((3, BLK, WIDE))

    outs = [shard(first) for first in (4, 4 + mid, low + 5, low + 5 + mid)]
    outs += [(whole, shaped((3, 3, BLK, WIDE))), (whole, shaped((4, 3, BLK, WIDE))), (pl.BlockSpec((8, 128), lambda j: (0, 0)), shaped((8, 128), F32))]
    sem = pltpu.SemaphoreType.DMA
    quarter = lambda *lead: pltpu.VMEM((*lead, 3, BLK, FT), BF16)
    scratch = [pltpu.VMEM((T, FT), BF16)] * 3
    scratch += [pltpu.VMEM((T, D), BF16)] * 2 + [pltpu.VMEM((D, T), BF16)] * 2 + [pltpu.VMEM((T, D), F32)]
    scratch += [quarter(2, 4), quarter(2, 4), quarter(3, 4), quarter(2, 2), quarter(2, 2), quarter(5, 2), quarter(2), quarter(2), quarter(5), quarter(mid)]
    scratch += [pltpu.VMEM((8, 128), F32), pltpu.VMEM((8, 8, 128), F32)]
    scratch += [sem((k,)) for k in (6, 2, 3, 2, 5, 2, 5, mid, mid, mid, mid, mid, mid, 7, 8, mid + 1, mid + 1)]
    return pl.pallas_call(
        kernel,
        grid_spec=pltpu.PrefetchScalarGridSpec(
            num_scalar_prefetch=0, grid=(steps,), in_specs=[whole] * 6 + [wdown, weight, weight, tile, tile], out_specs=[s for s, _ in outs], scratch_shapes=scratch
        ),
        out_shape=[o for _, o in outs],
        compiler_params=pltpu.CompilerParams(dimension_semantics=("arbitrary",), vmem_limit_bytes=63 * MB, collective_id=0, has_side_effects=True),
        cost_estimate=pl.CostEstimate(flops=12 * MM, bytes_accessed=120_000_000, transcendentals=0),
        name="backward",
    )(dy, a1, a1t, dyt, h, a0t, w_down, w_gate, w_up, gate, up)


def adamw(me, layer, first, width, base, factor, parts, w, m, v, so_far):
    ft = width
    steps, at0, part0 = width // ft, first // ft, (first - base) // ft

    def kernel(me_ref, f_ref, *refs):
        parts, refs = refs[:8], refs[8:]
        ws, ms, vs = refs[0:3], refs[3:6], refs[6:9]
        nws, nms, nvs, part = refs[-10:-7], refs[-7:-4], refs[-4:-1], refs[-1]
        f = f_ref[0:1, 0:1]
        p = pl.program_id(0)
        for at in range(8):

            @pl.when(p == at)
            def _(at=at):
                part[...] = parts[at][...]

        def take(i, rows, g):
            g = g.astype(F32) * f
            new_m = 0.9 * ms[i][0, rows, :] + 0.1 * g
            new_v = 0.95 * vs[i][0, rows, :] + 0.05 * g * g
            wide = ws[i][0, rows, :].astype(F32)
            nws[i][0, rows, :] = (wide - 0.02 * (new_m * lax.rsqrt(new_v + 1e-8) + 0.1 * wide)).astype(BF16)
            nms[i][0, rows, :] = new_m
            nvs[i][0, rows, :] = new_v

        for r in range(0, BLK, 16):
            for i in range(2):
                take(i, slice(r, r + 16), part[i, r : r + 16, :])
        for r in range(0, ft, 128):
            take(2, slice(r, r + 128), part[2, :, r : r + 128].T)

    def piece(at):
        where = lambda p, j: part0 + jnp.where(p == at, j, jnp.where(p < at, 0, steps - 1))
        if parts[at][1] is None:
            return pl.BlockSpec((3, BLK, ft), lambda p, j, me_ref: (0, 0, where(p, j)))
        return pl.BlockSpec((None, 3, BLK, ft), lambda p, j, me_ref: (parts[at][1], 0, 0, where(p, j)))

    across = pl.BlockSpec((1, BLK, ft), lambda p, j, me_ref: (layer, shard_at(p, me_ref[0]), at0 + j))
    along = pl.BlockSpec((1, ft, BLK), lambda p, j, me_ref: (layer, at0 + j, shard_at(p, me_ref[0])))
    three = [across, across, along]
    whole = pl.BlockSpec(memory_space=pl.ANY)
    ins = [pl.BlockSpec((8, 128), lambda p, j, me_ref: (0, 0))] + [piece(at) for at in range(8)] + three * 3
    args = [factor] + [a for a, _ in parts] + list(w) + list(m) + list(v)
    outs = [(s, shaped(o.shape, o.dtype)) for s, o in zip(three * 3, list(w) + list(m) + list(v))]
    aliases = {}
    if so_far is not None:
        aliases = {1 + len(ins) + i: i for i in range(9)}
        ins, args = ins + [whole] * 9, args + list(so_far)
    size = 3 * width * D
    return call(kernel, (8, steps), ins, outs, [pltpu.VMEM((3, BLK, ft), BF16)], flops=size * 200, moved=size * 22, aliases=aliases)(me, *args)


CORE = [(i, i ^ 1) for i in range(8)]
FIRST = [(i, i ^ (2 if i & 1 else 4)) for i in range(8)]
SECOND = [(i, i ^ (4 if i & 1 else 2)) for i in range(8)]


STAGES = {"core": CORE, "first": FIRST, "second": SECOND}


def swap(a, stage):
    return lax.ppermute(a, "dp", STAGES[stage])


def gather(own):
    mine = [own, swap(own, "second")]
    mine += [swap(a, "first") for a in mine]
    return [(a, None) for a in mine + [swap(a, "core") for a in mine]]


def solution(mesh):
    def work(x, dy, *arrays):
        weights, m, v = (arrays[i : i + 3] for i in (0, 3, 6))
        w_gate, w_up, w_down = weights
        x, dy = x[0], dy[0]
        me = lax.axis_index("dp").astype(jnp.int32).reshape(1)
        gate, up, h, a1, a1t, a0t, dyt = forward(me, x, dy, *weights)
        own1a, own1b, own0a, own0b, got, over, factor = backward(dy, a1, a1t, dyt, h, a0t, gate, up, *weights)

        parts = [(own1a, None)] + [(got, k) for k in range(3)] + [(over, k) for k in range(4)]
        new = None
        for first in (0, WIDE // 2):
            new = adamw(me, 1, first, WIDE // 2, 0, factor, parts, weights, m, v, new)
        for layer, number, own in ((1, 1, own1b), (0, 0, own0a), (0, 1, own0b)):
            parts = gather(own)
            new = adamw(me, layer, HALVES[number], WIDE, HALVES[number], factor, parts, weights, m, v, new)
        return tuple(new)

    return jax.shard_map(
        work,
        mesh=mesh,
        in_specs=(P(("rep", "dp"), None, None),) * 2 + (P(None, None, None),) * 9,
        out_specs=(P("rep", None, None),) * 9,
        check_vma=False,
    )
```
